16 devices in a mesh: model: 4 (over z, y), data: 4 (over x, core).
Axes of the slice: x: 2, y: 2, z: 2, core: 2. Of those that a mesh axis runs over, the one named last changes fastest.
Arguments:
- act_in: bfloat16 [32768, 1536], P('data')
- grad_out: bfloat16 [32768, 1536], P('data')
- w_up: bfloat16 [2, 1536, 6144], P(None, None, 'model')
- w_down: bfloat16 [2, 6144, 1536], P(None, 'model')
- master_up: float32 [2, 1536, 6144], P(None, 'data', 'model')
- master_down: float32 [2, 6144, 1536], P(None, ('model', 'data'))
- mom_up: float32 [2, 1536, 6144], P(None, 'data', 'model')
- mom_down: float32 [2, 6144, 1536], P(None, ('model', 'data'))
- var_up: float32 [2, 1536, 6144], P(None, 'data', 'model')
- var_down: float32 [2, 6144, 1536], P(None, ('model', 'data'))
- learn_rate: float32 [1], replicated
- clip_norm: float32 [1], replicated
Outputs:
- output 1: bfloat16 [2, 1536, 6144], P(None, None, 'model')
- output 2: bfloat16 [2, 6144, 1536], P(None, 'model')
- output 3: float32 [2, 1536, 6144], P(None, 'data', 'model')
- output 4: float32 [2, 6144, 1536], P(None, ('model', 'data'))
- output 5: float32 [2, 1536, 6144], P(None, 'data', 'model')
- output 6: float32 [2, 6144, 1536], P(None, ('model', 'data'))
- output 7: float32 [2, 1536, 6144], P(None, 'data', 'model')
- output 8: float32 [2, 6144, 1536], P(None, ('model', 'data'))
- output 9: float32 [1], replicated
All inputs are finite; a program needn't handle non-finite values.
Results may differ from the reference program's by a relative error of at most 0.00147203.
Values are sent between devices in bfloat16 or wider.
A program may use at most 1 GiB of HBM per device.

```python
import jax
import jax.numpy as jnp
from jax import lax

D = 1536
FF = 6144
TOKENS_DEV = 8192
DATA = 4
STEP = 10
ROWS = DATA * TOKENS_DEV

BETA_ONE = 0.9
BETA_TWO = 0.95
ADAM_EPS = 1e-8
NORM_EPS = 1e-6


def matmul(left_op, right_op):
    return jnp.dot(left_op, right_op, preferred_element_type=jnp.float32)


def gelu_fwd(z_low):
    return jax.nn.gelu(z_low.astype(jnp.float32)).astype(jnp.bfloat16)


def gelu_back(z_low, grad_low):
    _, back_fn = jax.vjp(jax.nn.gelu, z_low.astype(jnp.float32))
    return back_fn(grad_low.astype(jnp.float32))[0].astype(jnp.bfloat16)


def block_grads(x_blk, dy_blk, w_up, w_down):
    z_one = matmul(x_blk, w_up[0]).astype(jnp.bfloat16)
    act_one = gelu_fwd(z_one)
    hid_two = matmul(act_one, w_down[0]).astype(jnp.bfloat16)
    z_two = matmul(hid_two, w_up[1]).astype(jnp.bfloat16)
    act_two = gelu_fwd(z_two)
    grad_w4 = matmul(act_two.T, dy_blk)
    dact_two = matmul(dy_blk, w_down[1].T).astype(jnp.bfloat16)
    dz_two = gelu_back(z_two, dact_two)
    grad_w3 = matmul(hid_two.T, dz_two)
    dhid_two = matmul(dz_two, w_up[1].T).astype(jnp.bfloat16)
    grad_w2 = matmul(act_one.T, dhid_two)
    dact_one = matmul(dhid_two, w_down[0].T).astype(jnp.bfloat16)
    dz_one = gelu_back(z_one, dact_one)
    grad_w1 = matmul(x_blk.T, dz_one)
    return jnp.stack([grad_w1, grad_w3]), jnp.stack([grad_w2, grad_w4])


def adam_update(master_arr, mom_arr, var_arr, grad_arr, clip_scale, lr_val):
    scaled = clip_scale * grad_arr
    new_mom = BETA_ONE * mom_arr + (1.0 - BETA_ONE) * scaled
    new_var = BETA_TWO * var_arr + (1.0 - BETA_TWO) * scaled * scaled
    mom_hat = new_mom / (1.0 - BETA_ONE ** STEP)
    var_hat = new_var / (1.0 - BETA_TWO ** STEP)
    new_master = master_arr - lr_val * mom_hat / (jnp.sqrt(var_hat) + ADAM_EPS)
    return new_master, new_mom, new_var


def setup_inputs(seed: int = 0) -> dict:
    key_list = jax.random.split(jax.random.key(seed), 10)
    w_scale = D ** -0.5
    master_up = jax.random.normal(key_list[0], (2, D, FF), jnp.float32) * w_scale
    master_down = jax.random.normal(key_list[1], (2, FF, D), jnp.float32) * w_scale
    w_up = master_up.astype(jnp.bfloat16)
    w_down = master_down.astype(jnp.bfloat16)
    act_in = jax.random.normal(key_list[2], (ROWS, D), jnp.float32).astype(jnp.bfloat16)
    grad_out = jax.random.normal(key_list[3], (ROWS, D), jnp.float32).astype(jnp.bfloat16)
    est_up, est_down = block_grads(act_in[:TOKENS_DEV], grad_out[:TOKENS_DEV], w_up, w_down)
    sq_up = jnp.sum(est_up * est_up, axis=(1, 2)) / DATA
    sq_down = jnp.sum(est_down * est_down, axis=(1, 2)) / DATA
    est_norm = jnp.sqrt(jnp.sum(sq_up) + jnp.sum(sq_down))
    clip_frac = jax.random.uniform(key_list[4], (1,), jnp.float32, 0.3, 0.6)
    clip_norm = clip_frac * est_norm
    rms_up = clip_frac * jnp.sqrt(sq_up / (D * FF))
    rms_down = clip_frac * jnp.sqrt(sq_down / (D * FF))
    mom_up = jax.random.normal(key_list[5], (2, D, FF), jnp.float32) * rms_up[:, None, None]
    mom_down = jax.random.normal(key_list[6], (2, FF, D), jnp.float32) * rms_down[:, None, None]
    var_up = jax.random.uniform(key_list[7], (2, D, FF), jnp.float32, 0.25, 2.0) * (rms_up * rms_up)[:, None, None]
    var_down = jax.random.uniform(key_list[8], (2, FF, D), jnp.float32, 0.25, 2.0) * (rms_down * rms_down)[:, None, None]
    learn_rate = jax.random.uniform(key_list[9], (1,), jnp.float32, 0.1, 0.25) * w_scale
    return {"act_in": act_in, "grad_out": grad_out, "w_up": w_up, "w_down": w_down, "master_up": master_up, "master_down": master_down, "mom_up": mom_up, "mom_down": mom_down, "var_up": var_up, "var_down": var_down, "learn_rate": learn_rate, "clip_norm": clip_norm}


def reference(act_in, grad_out, w_up, w_down, master_up, master_down, mom_up, mom_down, var_up, var_down, learn_rate, clip_norm):
    x_blocks = act_in.reshape(DATA, TOKENS_DEV, D)
    dy_blocks = grad_out.reshape(DATA, TOKENS_DEV, D)

    def body_fn(carry_sum, block_pair):
        part_up, part_down = block_grads(block_pair[0], block_pair[1], w_up, w_down)
        return (carry_sum[0] + part_up, carry_sum[1] + part_down), None

    zero_sums = (jnp.zeros((2, D, FF), jnp.float32), jnp.zeros((2, FF, D), jnp.float32))
    grad_sums, _ = lax.scan(body_fn, zero_sums, (x_blocks, dy_blocks))
    grad_up = grad_sums[0] / DATA
    grad_down = grad_sums[1] / DATA
    sq_total = jnp.sum(grad_up * grad_up) + jnp.sum(grad_down * grad_down)
    norm_val = jnp.sqrt(sq_total)
    clip_scale = jnp.minimum(1.0, clip_norm[0] / (norm_val + NORM_EPS))
    lr_val = learn_rate[0]
    new_master_up, new_mom_up, new_var_up = adam_update(master_up, mom_up, var_up, grad_up, clip_scale, lr_val)
    new_master_down, new_mom_down, new_var_down = adam_update(master_down, mom_down, var_down, grad_down, clip_scale, lr_val)
    return (new_master_up.astype(jnp.bfloat16), new_master_down.astype(jnp.bfloat16), new_master_up, new_master_down, new_mom_up, new_mom_down, new_var_up, new_var_down, norm_val.reshape(1))
```

```python
import jax
import jax.numpy as jnp
from jax import lax
from jax.experimental import pallas as pl
from jax.experimental.pallas import tpu as pltpu
from jax.sharding import Mesh, PartitionSpec as P


STEP = 10
BETA_ONE = 0.9
BETA_TWO = 0.95
ADAM_EPS = 1e-8
NORM_EPS = 1e-6
DATA = 4


def gelu_fwd(z_low):
    return jax.nn.gelu(z_low.astype(jnp.float32)).astype(jnp.bfloat16)


def gelu_back(z_low, grad_low):
    _, back_fn = jax.vjp(jax.nn.gelu, z_low.astype(jnp.float32))
    return back_fn(grad_low.astype(jnp.float32))[0].astype(jnp.bfloat16)


def adam_kernel(scale_ref, lr_ref, master_ref, mom_ref, var_ref, grad_ref, *refs):
    out_master, out_mom, out_var, out_low = refs[-4:]
    scaled = scale_ref[0] * (grad_ref[...] / DATA)
    new_mom = BETA_ONE * mom_ref[0] + (1.0 - BETA_ONE) * scaled
    new_var = BETA_TWO * var_ref[0] + (1.0 - BETA_TWO) * scaled * scaled
    mom_hat = new_mom / (1.0 - BETA_ONE ** STEP)
    var_hat = new_var / (1.0 - BETA_TWO ** STEP)
    new_master = master_ref[0] - lr_ref[0] * mom_hat / (jnp.sqrt(var_hat) + ADAM_EPS)
    out_master[0], out_mom[0], out_var[0] = new_master, new_mom, new_var
    out_low[...] = new_master.astype(jnp.bfloat16)


def adam_update(layer, scale, lr_val, master, mom, var, grad, earlier):
    rows, cols = grad.shape
    tile = rows // 6
    smem = pl.BlockSpec(memory_space=pltpu.SMEM)
    slab = pl.BlockSpec((1, tile, cols), lambda i: (layer, i, 0))
    flat = pl.BlockSpec((tile, cols), lambda i: (i, 0))
    held = [pl.BlockSpec(memory_space=pl.ANY)] * len(earlier)
    count = master[0].size
    return pl.pallas_call(
        adam_kernel,
        grid=(6,),
        out_shape=[jax.ShapeDtypeStruct(master.shape, jnp.float32)] * 3 + [jax.ShapeDtypeStruct(grad.shape, jnp.bfloat16)],
        in_specs=[smem, smem, slab, slab, slab, flat] + held,
        out_specs=[slab, slab, slab, flat],
        input_output_aliases={6 + i: i for i in range(len(earlier))},
        cost_estimate=pl.CostEstimate(flops=20 * count, bytes_accessed=30 * count, transcendentals=count),
        name="adam",
    )(scale, lr_val, master, mom, var, grad, *earlier)


def swap(arr, axis):
    return lax.ppermute(arr, axis, [(0, 1), (1, 0)])


def gather_model(block):
    z_pos, y_pos, block = lax.optimization_barrier((lax.axis_index("z"), lax.axis_index("y"), block))
    half = block.shape[0] // 2
    top, bot = block[:half], block[half:]
    top_z, bot_y = swap(top, "z"), swap(bot, "y")
    top_y, bot_z = swap(top, "y"), swap(bot, "z")
    top_zy, bot_zy = swap(top_z, "y"), swap(bot_y, "z")
    rows, _ = block.shape
    full = jnp.concatenate([block] * 4, 0)
    for dz, dy, upper, lower in ((1, 0, top_z, bot_z), (0, 1, top_y, bot_y), (1, 1, top_zy, bot_zy)):
        place = 2 * (z_pos ^ dz) + (y_pos ^ dy)
        full = lax.dynamic_update_slice(full, upper, (place * rows, 0))
        full = lax.dynamic_update_slice(full, lower, (place * rows + half, 0))
    return full


def dot(left, right, dims):
    return lax.dot_general(left, right, (dims, ((), ())), preferred_element_type=jnp.float32)


def core_sum(part_own, part_oth):
    from_oth = swap(part_oth, "c")
    own = (lax.optimization_barrier(part_own) + from_oth).astype(jnp.bfloat16)
    return own, swap(own, "c")


def solution(mesh):
    mesh = Mesh(mesh.devices.reshape(2, 2, 2, 2), ("z", "y", "x", "c"))
    model, data = ("z", "y"), ("x", "c")
    spec_rows = P(data, None)
    spec_wup = P(None, None, model)
    spec_wdown = P(None, model, None)
    spec_sup = P(None, data, model)
    spec_sdown = P(None, model + data, None)
    spec_scalar = P(None)

    def whole_step(act_in, grad_out, w_up, w_down, master_up, master_down, mom_up, mom_down, var_up, var_down, learn_rate, clip_norm):
        core, x_pos = lax.axis_index("c"), lax.axis_index("x")
        quarter = 2 * lax.axis_index("z") + lax.axis_index("y")
        rows = act_in.shape[0] // 4
        dim = act_in.shape[1]
        piece = dim // 4

        def up_block(layer):
            parts = [lax.dynamic_slice(w_up, (layer, 0, (2 * i + core) * piece), (1, dim, piece))[0].T for i in range(2)]
            return jnp.concatenate(parts, 0)

        def down_block(layer):
            parts = [lax.dynamic_slice(w_down, (layer, (2 * i + core) * piece, 0), (1, piece, dim))[0] for i in range(2)]
            return jnp.concatenate(parts, 0)

        w_one = gather_model(up_block(0))
        x_own = lax.dynamic_slice_in_dim(act_in, quarter * rows, rows, 0)
        dy_own = lax.dynamic_slice_in_dim(grad_out, quarter * rows, rows, 0)
        x_oth, dy_oth = swap(x_own, "c"), swap(dy_own, "c")
        x_all = jnp.concatenate([x_own, x_oth], 0)
        dy_all = jnp.concatenate([dy_own, dy_oth], 0)
        w_two = gather_model(down_block(0))
        w_three = gather_model(up_block(1))
        w_four = gather_model(down_block(1))

        z_one_oth = dot(x_oth, w_one, ((1,), (1,))).astype(jnp.bfloat16)
        act_one_oth = gelu_fwd(z_one_oth)
        z_one_own = dot(x_own, w_one, ((1,), (1,))).astype(jnp.bfloat16)
        act_one_own = gelu_fwd(z_one_own)
        hid_oth = dot(act_one_oth, w_two, ((1,), (0,)))
        hid_own = dot(act_one_own, w_two, ((1,), (0,)))
        z_one = jnp.concatenate([z_one_own, z_one_oth], 0)
        act_one = jnp.concatenate([act_one_own, act_one_oth], 0)
        hid_own, hid_oth = core_sum(hid_own, hid_oth)
        hid_two = jnp.concatenate([hid_own, hid_oth], 0)
        z_two = dot(hid_two, w_three, ((1,), (1,))).astype(jnp.bfloat16)
        act_two = gelu_fwd(z_two)

        def scatter(grad):
            return lax.psum_scatter(grad, ("z", "y", "x"), scatter_dimension=0, tiled=True)

        def model_major(grad):
            return grad.reshape(dim, 4, 2 * piece).transpose(1, 0, 2).reshape(4 * dim, 2 * piece)

        def core_exchange(mine):
            mine = mine.reshape(2, piece, 2, piece)
            keep = lax.dynamic_index_in_dim(mine, core, 0, keepdims=False)
            give = lax.dynamic_index_in_dim(mine, 1 - core, 0, keepdims=False)
            got = swap(give, "c")
            pair = jnp.where(core == 0, jnp.stack([keep, got], 2), jnp.stack([got, keep], 2))
            return pair.reshape(piece, dim)

        grad_w4 = dot(act_two, dy_all, ((0,), (0,)))
        sum_w4 = scatter(grad_w4)
        dact_two = dot(dy_all, w_four, ((1,), (1,))).astype(jnp.bfloat16)
        dz_two = gelu_back(z_two, dact_two)
        grad_w3 = dot(hid_two, dz_two, ((0,), (0,)))
        sum_w3 = scatter(model_major(grad_w3))
        dhid_oth = dot(dz_two[rows:], w_three, ((1,), (0,)))
        dhid_own = dot(dz_two[:rows], w_three, ((1,), (0,)))
        dhid_own, dhid_oth = core_sum(dhid_own, dhid_oth)
        dhid_two = jnp.concatenate([dhid_own, dhid_oth], 0)
        grad_w2 = dot(act_one, dhid_two, ((0,), (0,)))
        sum_w2 = scatter(grad_w2)
        dact_one = dot(dhid_two, w_two, ((1,), (1,))).astype(jnp.bfloat16)
        dz_one = gelu_back(z_one, dact_one)
        grad_w1 = dot(x_all, dz_one, ((0,), (0,)))
        sum_w1 = scatter(model_major(grad_w1))

        total = jnp.zeros((1,), jnp.float32)
        for part in (sum_w4, sum_w3, sum_w2, sum_w1):
            total = total + jnp.sum((part / DATA) * (part / DATA))
        for axis in ("c", "x", "y", "z"):
            total = total + swap(total, axis)
        norm_val = jnp.sqrt(total)
        clip_scale = jnp.minimum(1.0, clip_norm[0] / (norm_val[0] + NORM_EPS))
        sum_w1, sum_w3 = core_exchange(sum_w1), core_exchange(sum_w3)

        new_w_up = jnp.zeros((2, dim, dim), jnp.bfloat16)
        new_w_down = jnp.zeros((2, dim, dim), jnp.bfloat16)
        scale = clip_scale.reshape(1)
        up, down = (), ()
        for name, layer, grad in (("down", 1, sum_w4), ("up", 1, sum_w3), ("down", 0, sum_w2), ("up", 0, sum_w1)):
            if name == "up":
                *up, low = adam_update(layer, scale, learn_rate, master_up, mom_up, var_up, grad, up)
            else:
                *down, low = adam_update(layer, scale, learn_rate, master_down, mom_down, var_down, grad, down)
            far = swap(low, "x")
            near, far_near = swap(low, "c"), swap(far, "c")
            for dx, dc, part in ((0, 0, low), (0, 1, near), (1, 0, far), (1, 1, far_near)):
                place = (layer, (2 * (x_pos ^ dx) + (core ^ dc)) * piece, 0)
                if name == "up":
                    new_w_up = lax.dynamic_update_slice(new_w_up, part[None], place)
                else:
                    new_w_down = lax.dynamic_update_slice(new_w_down, part[None], place)
        (new_master_up, new_mom_up, new_var_up), (new_master_down, new_mom_down, new_var_down) = up, down
        return (new_w_up, new_w_down, new_master_up, new_master_down, new_mom_up, new_mom_down, new_var_up, new_var_down, norm_val)

    return jax.shard_map(whole_step, mesh=mesh, in_specs=(spec_rows, spec_rows, spec_wup, spec_wdown, spec_sup, spec_sdown, spec_sup, spec_sdown, spec_sup, spec_sdown, spec_scalar, spec_scalar), out_specs=(spec_wup, spec_wdown, spec_sup, spec_sdown, spec_sup, spec_sdown, spec_sup, spec_sdown, spec_scalar), check_vma=False)
```

```python
import math

import jax
import jax.numpy as jnp
from jax import lax
from jax.experimental import pallas as pl
from jax.experimental.pallas import tpu as pltpu
from jax.sharding import Mesh, PartitionSpec as P


STEP = 10
BETA_ONE = 0.9
BETA_TWO = 0.95
ADAM_EPS = 1e-8
NORM_EPS = 1e-6
DATA = 4
AXES = ("z", "y", "x", "c")
GELU_A = (2.0 / math.pi) ** 0.5
GELU_B = 0.044715 * GELU_A


def gelu_fwd(z_low):
    return jax.nn.gelu(z_low.astype(jnp.float32)).astype(jnp.bfloat16)


def gelu_back(z_low, grad_low):
    z, grad = z_low.astype(jnp.float32), grad_low.astype(jnp.float32)
    square = z * z
    tanh = jnp.tanh(z * (GELU_A + GELU_B * square))
    slope = (0.5 + 0.5 * tanh) + z * (1.0 - tanh * tanh) * (0.5 * GELU_A + 1.5 * GELU_B * square)
    return (grad * slope).astype(jnp.bfloat16)


def norm_kernel(part_ref, total_ref, held, send_sem, recv_sem):
    here = [lax.axis_index(axis) for axis in AXES]
    place = lambda spot: 8 * spot[0] + 4 * spot[1] + 2 * spot[2] + spot[3]
    peers = [[1 - pos if step >> (3 - i) & 1 else pos for i, pos in enumerate(here)] for step in range(1, 16)]
    barrier = pltpu.get_barrier_semaphore()
    for peer in peers:
        pl.semaphore_signal(barrier, inc=1, device_id=tuple(peer), device_id_type=pl.DeviceIdType.MESH)
    pl.semaphore_wait(barrier, 15)
    held[place(here)] = part_ref[...]

    def copy(step, peer, slot):
        return pltpu.make_async_remote_copy(
            src_ref=part_ref,
            dst_ref=held.at[slot],
            send_sem=send_sem.at[step],
            recv_sem=recv_sem.at[slot],
            device_id=tuple(peer),
            device_id_type=pl.DeviceIdType.MESH,
        )

    for step, peer in enumerate(peers):
        copy(step, peer, place(here)).start()
    for step, peer in enumerate(peers):
        copy(step, peer, place(here)).wait_send()
        copy(step, peer, place(peer)).wait_recv()
    total = held[0]
    for slot in range(1, 16):
        total = total + held[slot]
    total_ref[...] = total


def norm_sum(part):
    vmem = pl.BlockSpec(memory_space=pltpu.VMEM)
    return pl.pallas_call(
        norm_kernel,
        out_shape=jax.ShapeDtypeStruct((8, 128), jnp.float32),
        in_specs=[vmem],
        out_specs=vmem,
        scratch_shapes=[pltpu.VMEM((16, 8, 128), jnp.float32), pltpu.SemaphoreType.DMA((15,)), pltpu.SemaphoreType.DMA((16,))],
        compiler_params=pltpu.CompilerParams(collective_id=0, has_side_effects=True),
        name="norm",
    )(jnp.broadcast_to(part, (8, 128)))[0, :1]


def adam_kernel(scale_ref, lr_ref, master_ref, mom_ref, var_ref, grad_ref, *refs):
    out_master, out_mom, out_var, out_low = refs[-4:]
    scaled = scale_ref[0] * (grad_ref[...] / DATA)
    new_mom = BETA_ONE * mom_ref[0] + (1.0 - BETA_ONE) * scaled
    new_var = BETA_TWO * var_ref[0] + (1.0 - BETA_TWO) * scaled * scaled
    mom_hat = new_mom / (1.0 - BETA_ONE ** STEP)
    var_hat = new_var / (1.0 - BETA_TWO ** STEP)
    new_master = master_ref[0] - lr_ref[0] * mom_hat / (jnp.sqrt(var_hat) + ADAM_EPS)
    out_master[0], out_mom[0], out_var[0] = new_master, new_mom, new_var
    out_low[...] = new_master.astype(jnp.bfloat16)


def adam_update(layer, scale, lr_val, master, mom, var, grad, earlier):
    rows, cols = grad.shape
    tile = rows // 6
    smem = pl.BlockSpec(memory_space=pltpu.SMEM)
    slab = pl.BlockSpec((1, tile, cols), lambda i: (layer, i, 0))
    flat = pl.BlockSpec((tile, cols), lambda i: (i, 0))
    held = [pl.BlockSpec(memory_space=pl.ANY)] * len(earlier)
    count = master[0].size
    return pl.pallas_call(
        adam_kernel,
        grid=(6,),
        out_shape=[jax.ShapeDtypeStruct(master.shape, jnp.float32)] * 3 + [jax.ShapeDtypeStruct(grad.shape, jnp.bfloat16)],
        in_specs=[smem, smem, slab, slab, slab, flat] + held,
        out_specs=[slab, slab, slab, flat],
        input_output_aliases={6 + i: i for i in range(len(earlier))},
        cost_estimate=pl.CostEstimate(flops=20 * count, bytes_accessed=30 * count, transcendentals=count),
        name="adam",
    )(scale, lr_val, master, mom, var, grad, *earlier)


def swap(arr, axis):
    return lax.ppermute(arr, axis, [(0, 1), (1, 0)])


def gather_model(block):
    z_pos, y_pos, block = lax.optimization_barrier((lax.axis_index("z"), lax.axis_index("y"), block))
    half = block.shape[0] // 2
    top, bot = block[:half], block[half:]
    top_z, bot_y = swap(top, "z"), swap(bot, "y")
    top_y, bot_z = swap(top, "y"), swap(bot, "z")
    top_zy, bot_zy = swap(top_z, "y"), swap(bot_y, "z")
    rows, _ = block.shape
    full = jnp.concatenate([block] * 4, 0)
    for dz, dy, upper, lower in ((1, 0, top_z, bot_z), (0, 1, top_y, bot_y), (1, 1, top_zy, bot_zy)):
        place = 2 * (z_pos ^ dz) + (y_pos ^ dy)
        full = lax.dynamic_update_slice(full, upper, (place * rows, 0))
        full = lax.dynamic_update_slice(full, lower, (place * rows + half, 0))
    return full


def dot(left, right, dims):
    return lax.dot_general(left, right, (dims, ((), ())), preferred_element_type=jnp.float32)


def core_sum(part_own, part_oth):
    from_oth = swap(part_oth, "c")
    own = (lax.optimization_barrier(part_own) + from_oth).astype(jnp.bfloat16)
    return own, swap(own, "c")


def solution(mesh):
    mesh = Mesh(mesh.devices.reshape(2, 2, 2, 2), ("z", "y", "x", "c"))
    model, data = ("z", "y"), ("x", "c")
    spec_rows = P(data, None)
    spec_wup = P(None, None, model)
    spec_wdown = P(None, model, None)
    spec_sup = P(None, data, model)
    spec_sdown = P(None, model + data, None)
    spec_scalar = P(None)

    def whole_step(act_in, grad_out, w_up, w_down, master_up, master_down, mom_up, mom_down, var_up, var_down, learn_rate, clip_norm):
        core, x_pos = lax.axis_index("c"), lax.axis_index("x")
        quarter = 2 * lax.axis_index("z") + lax.axis_index("y")
        rows = act_in.shape[0] // 4
        dim = act_in.shape[1]
        piece = dim // 4

        def up_block(layer):
            parts = [lax.dynamic_slice(w_up, (layer, 0, (2 * i + core) * piece), (1, dim, piece))[0].T for i in range(2)]
            return jnp.concatenate(parts, 0)

        def down_block(layer):
            parts = [lax.dynamic_slice(w_down, (layer, (2 * i + core) * piece, 0), (1, piece, dim))[0] for i in range(2)]
            return jnp.concatenate(parts, 0)

        w_one = gather_model(up_block(0))
        x_own = lax.dynamic_slice_in_dim(act_in, quarter * rows, rows, 0)
        dy_own = lax.dynamic_slice_in_dim(grad_out, quarter * rows, rows, 0)
        x_oth, dy_oth = swap(x_own, "c"), swap(dy_own, "c")
        x_all = jnp.concatenate([x_own, x_oth], 0)
        dy_all = jnp.concatenate([dy_own, dy_oth], 0)
        w_two = gather_model(down_block(0))

        z_one_oth = dot(x_oth, w_one, ((1,), (1,))).astype(jnp.bfloat16)
        act_one_oth = gelu_fwd(z_one_oth)
        z_one_own = dot(x_own, w_one, ((1,), (1,))).astype(jnp.bfloat16)
        act_one_own = gelu_fwd(z_one_own)
        share = lambda block: lax.dynamic_slice_in_dim(block, x_pos * piece, piece, 0)
        share_three, share_four, z_one_own, act_one_own = lax.optimization_barrier((share(up_block(1)), share(down_block(1)), z_one_own, act_one_own))
        w_three = lax.all_gather(share_three, ("z", "y", "x"), axis=0, tiled=True)
        w_four = lax.all_gather(share_four, ("z", "y", "x"), axis=0, tiled=True)
        hid_oth = dot(act_one_oth, w_two, ((1,), (0,)))
        hid_own = dot(act_one_own, w_two, ((1,), (0,)))
        z_one = jnp.concatenate([z_one_own, z_one_oth], 0)
        act_one = jnp.concatenate([act_one_own, act_one_oth], 0)
        hid_own, hid_oth = core_sum(hid_own, hid_oth)
        hid_two = jnp.concatenate([hid_own, hid_oth], 0)
        z_two = dot(hid_two, w_three, ((1,), (1,))).astype(jnp.bfloat16)
        act_two = gelu_fwd(z_two)

        def scatter(grad):
            return lax.psum_scatter(grad, ("z", "y", "x"), scatter_dimension=0, tiled=True)

        def model_major(grad):
            return grad.reshape(dim, 4, 2 * piece).transpose(1, 0, 2).reshape(4 * dim, 2 * piece)

        def core_exchange(mine):
            mine, core = lax.optimization_barrier((mine, lax.axis_index("c")))
            keep = lax.dynamic_slice_in_dim(mine, core * piece, piece, 0)
            give = lax.dynamic_slice_in_dim(mine, (1 - core) * piece, piece, 0)
            got = swap(give, "c")
            low, high = jnp.where(core == 0, keep, got), jnp.where(core == 0, got, keep)
            return jnp.concatenate([low[:, :piece], high[:, :piece], low[:, piece:], high[:, piece:]], 1)

        grad_w4 = dot(act_two, dy_all, ((0,), (0,)))
        sum_w4 = scatter(grad_w4)
        dact_two = dot(dy_all, w_four, ((1,), (1,))).astype(jnp.bfloat16)
        dz_two = gelu_back(z_two, dact_two)
        grad_w3 = dot(hid_two, dz_two, ((0,), (0,)))
        sum_w3 = scatter(model_major(grad_w3))
        dhid_oth = dot(dz_two[rows:], w_three, ((1,), (0,)))
        dhid_own = dot(dz_two[:rows], w_three, ((1,), (0,)))
        dhid_own, dhid_oth = core_sum(dhid_own, dhid_oth)
        dhid_two = jnp.concatenate([dhid_own, dhid_oth], 0)
        grad_w2 = dot(act_one, dhid_two, ((0,), (0,)))
        sum_w2 = scatter(grad_w2)
        dact_one = dot(dhid_two, w_two, ((1,), (1,))).astype(jnp.bfloat16)
        dz_one = gelu_back(z_one, dact_one)
        grad_w1 = dot(x_all, dz_one, ((0,), (0,)))
        sum_w1 = scatter(model_major(grad_w1))

        total = jnp.zeros((1,), jnp.float32)
        for part in (sum_w4, sum_w3, sum_w2, sum_w1):
            total = total + jnp.sum((part / DATA) * (part / DATA))
        total = norm_sum(total)
        norm_val = jnp.sqrt(total)
        clip_scale = jnp.minimum(1.0, clip_norm[0] / (norm_val[0] + NORM_EPS))
        sum_w1, sum_w3 = core_exchange(sum_w1), core_exchange(sum_w3)

        new_w_up = jnp.zeros((2, dim, dim), jnp.bfloat16)
        new_w_down = jnp.zeros((2, dim, dim), jnp.bfloat16)
        scale = clip_scale.reshape(1)
        up, down = (), ()
        for name, layer, grad in (("down", 1, sum_w4), ("up", 1, sum_w3), ("down", 0, sum_w2), ("up", 0, sum_w1)):
            if name == "up":
                *up, low = adam_update(layer, scale, learn_rate, master_up, mom_up, var_up, grad, up)
            else:
                *down, low = adam_update(layer, scale, learn_rate, master_down, mom_down, var_down, grad, down)
            far = swap(low, "x")
            near, far_near = swap(low, "c"), swap(far, "c")
            for dx, dc, part in ((0, 0, low), (0, 1, near), (1, 0, far), (1, 1, far_near)):
                place = (layer, (2 * (x_pos ^ dx) + (core ^ dc)) * piece, 0)
                if name == "up":
                    new_w_up = lax.dynamic_update_slice(new_w_up, part[None], place)
                else:
                    new_w_down = lax.dynamic_update_slice(new_w_down, part[None], place)
        (new_master_up, new_mom_up, new_var_up), (new_master_down, new_mom_down, new_var_down) = up, down
        return (new_w_up, new_w_down, new_master_up, new_master_down, new_mom_up, new_mom_down, new_var_up, new_var_down, norm_val)

    return jax.shard_map(whole_step, mesh=mesh, in_specs=(spec_rows, spec_rows, spec_wup, spec_wdown, spec_sup, spec_sdown, spec_sup, spec_sdown, spec_sup, spec_sdown, spec_scalar, spec_scalar), out_specs=(spec_wup, spec_wdown, spec_sup, spec_sdown, spec_sup, spec_sdown, spec_sup, spec_sdown, spec_scalar), check_vma=False)
```
